16 devices in a mesh: dp: 2 (over y, z), tp: 8 (over x, core).
Axes of the slice: x: 4, y: 2, z: 1, core: 2. Of those that a mesh axis runs over, the one named last changes fastest.
The devices are a block of a 4x4x8 slice.
Arguments:
- x_a: bfloat16 [4096, 4608], P(('dp', 'tp')), parts along dimension 0
- x_b: bfloat16 [4096, 4608], P(('dp', 'tp')), parts along dimension 0
- labels_a: int32 [4096], P(('dp', 'tp')), parts along dimension 0
- labels_b: int32 [4096], P(('dp', 'tp')), parts along dimension 0
- w_head: bfloat16 [4608, 49152], P(None, 'tp')
Outputs:
- output 1: float32 [4], P('dp'), parts along dimension 0
- output 2: bfloat16 [9216, 49152], P('dp', 'tp'), parts along dimension 0
- output 3: bfloat16 [4096, 4608], P(('dp', 'tp')), parts along dimension 0
- output 4: bfloat16 [4096, 4608], P(('dp', 'tp')), parts along dimension 0
There are 2 independent parts. The reference program is written for one: setup_inputs(seed, part) draws one part's arguments, and reference() takes and returns one part's arrays. A program takes and returns all parts, laid end to end along the dimension named above; an argument that names none is the same for every part.
All inputs are finite; a program needn't handle non-finite values.
Results may differ from the reference program's by a relative error of at most 0.001.
Values are sent between devices in bfloat16 or wider.
A program may use at most 768 MiB of HBM per device.

```python
import math
import jax
import jax.numpy as jnp
from jax import lax

TOKENS = 2048
HIDDEN = 4608
VOCAB = 49152
VOCAB_SPLIT = 8


def draw_labels(label_key):
    value_key, first_key, gap_key = jax.random.split(label_key, 3)
    label_ids = jax.random.randint(value_key, (TOKENS,), 0, VOCAB, jnp.int32)
    first_pos = jax.random.randint(first_key, (), 0, TOKENS, jnp.int32)
    second_pos = (first_pos + jax.random.randint(gap_key, (), 1, TOKENS, jnp.int32)) % TOKENS
    return label_ids.at[first_pos].set(0).at[second_pos].set(VOCAB - 1)


def setup_inputs(seed: int = 0, part: int = 0) -> dict:
    part_key = jax.random.fold_in(jax.random.key(seed), part)
    key_xa, key_xb, key_la, key_lb = jax.random.split(part_key, 4)
    x_a = jax.random.normal(key_xa, (TOKENS, HIDDEN), jnp.float32).astype(jnp.bfloat16)
    x_b = jax.random.normal(key_xb, (TOKENS, HIDDEN), jnp.float32).astype(jnp.bfloat16)
    w_scale = 2.5 / math.sqrt(HIDDEN)
    w_head = (jax.random.normal(jax.random.key(seed + 1), (HIDDEN, VOCAB), jnp.float32) * w_scale).astype(jnp.bfloat16)
    return {"x_a": x_a, "x_b": x_b, "labels_a": draw_labels(key_la), "labels_b": draw_labels(key_lb), "w_head": w_head}


def reference(x_a, x_b, labels_a, labels_b, w_head):
    shard_cols = VOCAB // VOCAB_SPLIT
    w_blocks = w_head.reshape(HIDDEN, VOCAB_SPLIT, shard_cols).transpose(1, 0, 2)
    offsets = jnp.arange(VOCAB_SPLIT, dtype=jnp.int32) * shard_cols
    x_flat = jnp.concatenate([x_a, x_b], axis=0)
    label_flat = jnp.concatenate([labels_a, labels_b], axis=0)
    col_ids = jnp.arange(shard_cols, dtype=jnp.int32)[None, :]

    def block_stats(block_args):
        w_block, offset = block_args
        logits = jnp.dot(x_flat, w_block, preferred_element_type=jnp.float32)
        block_max = jnp.max(logits, axis=1)
        block_sum = jnp.sum(jnp.exp(logits - block_max[:, None]), axis=1)
        label_hit = col_ids == (label_flat - offset)[:, None]
        block_target = jnp.sum(jnp.where(label_hit, logits, 0.0), axis=1)
        return block_max, block_sum, block_target

    all_max, all_sum, all_target = lax.map(block_stats, (w_blocks, offsets))
    row_max = jnp.max(all_max, axis=0)
    row_sum = jnp.sum(all_sum * jnp.exp(all_max - row_max[None, :]), axis=0)
    target = jnp.sum(all_target, axis=0)
    loss_tok = row_max + jnp.log(row_sum) - target
    losses = jnp.stack([jnp.mean(loss_tok[:TOKENS]), jnp.mean(loss_tok[TOKENS:])])

    def block_grad(dx_acc, block_args):
        w_block, offset = block_args
        logits = jnp.dot(x_flat, w_block, preferred_element_type=jnp.float32)
        label_hit = col_ids == (label_flat - offset)[:, None]
        probs = jnp.exp(logits - row_max[:, None]) / row_sum[:, None]
        grad_logits = ((probs - label_hit.astype(jnp.float32)) / TOKENS).astype(jnp.bfloat16)
        grad_block = jnp.dot(x_flat.T, grad_logits, preferred_element_type=jnp.float32).astype(jnp.bfloat16)
        dx_acc = dx_acc + jnp.dot(grad_logits, w_block.T, preferred_element_type=jnp.float32)
        return dx_acc, grad_block

    dx_init = jnp.zeros((2 * TOKENS, HIDDEN), jnp.float32)
    dx_sum, grad_blocks = lax.scan(block_grad, dx_init, (w_blocks, offsets))
    grad_w = grad_blocks.transpose(1, 0, 2).reshape(HIDDEN, VOCAB)
    grad_x = dx_sum.astype(jnp.bfloat16)
    return losses, grad_w, grad_x[:TOKENS], grad_x[TOKENS:]
```

```python
import functools

import jax
import jax.numpy as jnp
from jax import lax
from jax.experimental import pallas as pl
from jax.experimental.pallas import tpu as pltpu
from jax.sharding import PartitionSpec as P

F32 = jnp.float32
BF16 = jnp.bfloat16
LOWEST = -3.4028235e38
VMEM_BYTES = 67043328
LANES = 128
CHIPS = 4
PHASES = 2 * CHIPS
LOGIT_COLS, LOGIT_SUB = 1024, 512
G_ROWS, G_COLS, X_TILE, X_SUB, PART = 1024, 768, 512, 512, 32
PARTNER, RIGHT, LEFT, FORWARD_RIGHT, FORWARD_LEFT, PASS_RIGHT, PASS_LEFT, PASS_FIRST, PASS_SECOND = range(9)


def phase_block(phase, chip):
    turn = lax.rem(phase + 1, 3)
    away = lax.min(lax.div(phase, 2), 1) * (1 + 2 * turn - 3 * lax.div(turn, 2))
    batch = lax.div(phase, 5) + 1 - lax.min((phase - 1) * (phase - 1), 1)
    return batch, lax.rem(chip + away, CHIPS)


def logits_kernel(
    x_a, x_b, lab, w_ref, z_ref, x_full, lab_full, stat_full,
    x_buf, run_max, run_sum, stat,
    send_sem, recv_sem, lab_send, lab_recv, stat_send, stat_recv, own_sem, keep_sem, load_sem,
    *, group, sub,
):
    phase, step = pl.program_id(0), pl.program_id(1)
    steps = pl.num_programs(1)
    rows, cols = z_ref.shape
    unit = x_a.shape[0]
    half = unit // 2
    tokens = unit * group
    me = lax.axis_index("tp")
    chip, core = lax.div(me, 2), lax.rem(me, 2)
    partner = chip * 2 + 1 - core
    device = lambda hops: lax.rem(chip + hops, CHIPS) * 2 + core
    right, opposite, left = device(1), device(2), device(3)
    x_own = (x_a, x_b)

    def rows_of(batch, dev, first=0, size=unit):
        return x_full.at[pl.ds(pl.multiple_of(batch * tokens + dev * unit + first, half), size)]

    def copy(kind, batch):
        src = dst = None
        if kind == PARTNER:
            src, to = x_own[batch], partner
            dst = x_buf.at[batch, pl.ds(pl.multiple_of(core * unit, half), unit)]
        elif kind in (RIGHT, LEFT):
            src, to = x_own[batch], right if kind == RIGHT else left
            dst = rows_of(batch, me)
        elif kind == FORWARD_RIGHT:
            src, to = rows_of(batch, left, 0, half), right
        elif kind == FORWARD_LEFT:
            src, to = rows_of(batch, right, half, half), left
        elif kind == PASS_RIGHT:
            src, to = rows_of(batch, right), partner
        elif kind == PASS_LEFT:
            src, to = rows_of(batch, left), partner
        elif kind == PASS_FIRST:
            src, to = rows_of(batch, opposite, 0, half), partner
        else:
            src, to = rows_of(batch, opposite, half, half), partner
        return pltpu.make_async_remote_copy(
            src_ref=src, dst_ref=src if dst is None else dst,
            send_sem=send_sem.at[kind, batch], recv_sem=recv_sem.at[kind, batch],
            device_id={"tp": to}, device_id_type=pl.DeviceIdType.MESH,
        )

    def label_copy(k):
        return pltpu.make_async_remote_copy(
            src_ref=lab, dst_ref=lab_full.at[me], send_sem=lab_send.at[k], recv_sem=lab_recv.at[k],
            device_id={"tp": lax.rem(me + k, group)}, device_id_type=pl.DeviceIdType.MESH,
        )

    def stat_copy(batch, k):
        return pltpu.make_async_remote_copy(
            src_ref=stat.at[batch], dst_ref=stat_full.at[me, batch],
            send_sem=stat_send.at[batch, k], recv_sem=stat_recv.at[batch, k],
            device_id={"tp": lax.rem(me + k, group)}, device_id_type=pl.DeviceIdType.MESH,
        )

    def own_load(batch):
        return pltpu.make_async_copy(
            x_own[batch], x_buf.at[batch, pl.ds(pl.multiple_of(core * unit, half), unit)], own_sem.at[batch]
        )

    def own_keep(batch):
        return pltpu.make_async_copy(x_buf.at[batch], rows_of(batch, chip * 2, 0, 2 * unit), keep_sem.at[batch])

    def load(to_phase):
        batch, away = phase_block(jnp.int32(to_phase), chip)
        return pltpu.make_async_copy(rows_of(batch, away * 2, 0, 2 * unit), x_buf.at[to_phase % 2], load_sem)

    label_own = pltpu.make_async_copy(lab, lab_full.at[me], own_sem.at[2])
    stat_own = lambda batch: pltpu.make_async_copy(stat.at[batch], stat_full.at[me, batch], own_sem.at[3 + batch])
    at = lambda p, s: pl.when((phase == p) & (step == s))
    last = steps - 1
    others = range(1, group)

    @at(0, 0)
    def _():
        barrier = pltpu.get_barrier_semaphore()
        for k in others:
            pl.semaphore_signal(
                barrier, inc=1, device_id={"tp": lax.rem(me + k, group)}, device_id_type=pl.DeviceIdType.MESH
            )
        own_load(0).start()
        own_load(1).start()
        pl.semaphore_wait(barrier, group - 1)
        copy(PARTNER, 0).start()
        copy(RIGHT, 0).start()
        copy(LEFT, 0).start()
        copy(PARTNER, 1).start()
        for k in others:
            label_copy(k).start()
        label_own.start()
        own_load(0).wait()
        copy(PARTNER, 0).wait_recv()
        own_keep(0).start()

    @at(0, last)
    def _():
        own_load(1).wait()
        copy(PARTNER, 1).wait_recv()
        own_keep(1).start()

    def arrived(batch):
        copy(RIGHT, batch).wait_recv()
        copy(LEFT, batch).wait_recv()
        copy(FORWARD_RIGHT, batch).start()
        copy(FORWARD_LEFT, batch).start()
        copy(PASS_RIGHT, batch).start()
        copy(PASS_LEFT, batch).start()

    def arrived_far(batch):
        copy(FORWARD_RIGHT, batch).wait_recv()
        copy(FORWARD_LEFT, batch).wait_recv()
        copy(PASS_FIRST, batch).start()
        copy(PASS_SECOND, batch).start()

    @at(1, (7 * steps) // 12)
    def _():
        arrived(0)
        copy(RIGHT, 1).start()
        copy(LEFT, 1).start()

    @at(1, last)
    def _():
        own_keep(0).wait()
        copy(PASS_RIGHT, 0).wait_recv()
        load(2).start()

    @at(2, (8 * steps) // 12)
    def _():
        arrived_far(0)

    @at(2, last)
    def _():
        own_keep(1).wait()
        copy(PASS_LEFT, 0).wait_recv()
        load(3).start()

    @at(3, last)
    def _():
        copy(PASS_FIRST, 0).wait_recv()
        copy(PASS_SECOND, 0).wait_recv()
        load(4).start()

    @at(4, (4 * steps) // 12)
    def _():
        arrived(1)

    @at(4, last)
    def _():
        copy(PASS_RIGHT, 1).wait_recv()
        load(5).start()

    @at(5, 1)
    def _():
        for k in others:
            stat_copy(0, k).start()
        stat_own(0).start()

    @at(5, (6 * steps) // 12)
    def _():
        arrived_far(1)

    @at(5, last)
    def _():
        copy(PASS_LEFT, 1).wait_recv()
        load(6).start()

    @at(6, last)
    def _():
        copy(PASS_FIRST, 1).wait_recv()
        copy(PASS_SECOND, 1).wait_recv()
        load(7).start()

    @pl.when((step == 0) & (phase >= 2))
    def _():
        load(2).wait()

    @pl.when(step == 0)
    def _():
        run_max[...] = jnp.full_like(run_max, LOWEST)
        run_sum[...] = jnp.zeros_like(run_sum)

    x = x_buf.at[lax.rem(phase, 2)]
    for r in range(0, rows, sub):
        tile = jnp.dot(x[r : r + sub, :], w_ref[...], preferred_element_type=F32)
        z_ref[r : r + sub, :] = tile
        old = run_max[r : r + sub, :]
        new = old
        for c in range(0, cols, LANES):
            new = jnp.maximum(new, tile[:, c : c + LANES])
        total = run_sum[r : r + sub, :] * jnp.exp(old - new)
        for c in range(0, cols, LANES):
            total = total + jnp.exp(tile[:, c : c + LANES] - new)
        run_max[r : r + sub, :] = new
        run_sum[r : r + sub, :] = total

    @pl.when(step == last)
    def _():
        batch, away = phase_block(phase, chip)
        spot = pl.ds(pl.multiple_of(away * rows, rows), rows)
        lane_max = run_max[...].T
        top = jnp.max(lane_max, axis=0, keepdims=True)
        stat[batch, 0:1, spot] = top
        stat[batch, 1:2, spot] = jnp.sum(run_sum[...].T * jnp.exp(lane_max - top), axis=0, keepdims=True)

    @at(PHASES - 1, last)
    def _():
        for kind in range(9):
            for batch in range(2):
                copy(kind, batch).wait_send()
        for k in others:
            label_copy(k).wait()
        label_own.wait()
        for k in others:
            stat_copy(1, k).start()
        stat_own(1).start()
        for batch in range(2):
            for k in others:
                stat_copy(batch, k).wait()
            stat_own(batch).wait()


def gather_logits(x_a, x_b, lab, w, group):
    unit, hidden = x_a.shape
    vocab = w.shape[1]
    tokens = unit * group
    rows, cols, sub = 2 * unit, LOGIT_COLS, LOGIT_SUB

    def z_block(phase, step):
        batch, away = phase_block(phase, lax.div(lax.axis_index("tp"), 2))
        return batch * CHIPS + away, step

    hbm = pl.BlockSpec(memory_space=pl.ANY)
    dma = pltpu.SemaphoreType.DMA
    return pl.pallas_call(
        functools.partial(logits_kernel, group=group, sub=sub),
        grid=(PHASES, vocab // cols),
        in_specs=[hbm, hbm, hbm, pl.BlockSpec((hidden, cols), lambda p, n: (0, n))],
        out_specs=[pl.BlockSpec((rows, cols), z_block), hbm, hbm, hbm],
        out_shape=[
            jax.ShapeDtypeStruct((2 * tokens, vocab), F32),
            jax.ShapeDtypeStruct((2 * tokens, hidden), BF16),
            jax.ShapeDtypeStruct((group, 2, unit), jnp.int32),
            jax.ShapeDtypeStruct((group, 2, 2, tokens), F32),
        ],
        scratch_shapes=[
            pltpu.VMEM((2, rows, hidden), BF16),
            pltpu.VMEM((rows, LANES), F32),
            pltpu.VMEM((rows, LANES), F32),
            pltpu.VMEM((2, 2, tokens), F32),
            dma((9, 2)), dma((9, 2)), dma((group,)), dma((group,)), dma((2, group)), dma((2, group)),
            dma((5,)), dma((2,)), dma,
        ],
        compiler_params=pltpu.CompilerParams(
            vmem_limit_bytes=VMEM_BYTES, collective_id=0, has_side_effects=True,
            dimension_semantics=("arbitrary", "arbitrary"),
        ),
        cost_estimate=pl.CostEstimate(
            flops=4 * tokens * hidden * vocab, bytes_accessed=8 * tokens * vocab, transcendentals=0
        ),
        name="gather_logits",
    )(x_a, x_b, lab, w)


def grad_x_kernel(*refs, first, blocks, inv_tokens, resume):
    if resume:
        z_ref, w_ref, top_ref, inv_ref, lab_ref, g_in, g_ref, dx_ref, hit_ref, g_even, g_odd, hits, sem = refs
    else:
        z_ref, w_ref, top_ref, inv_ref, lab_ref, g_ref, dx_ref, hit_ref, g_even, g_odd, hits = refs
    block, step = pl.program_id(0), pl.program_id(1)
    steps = pl.num_programs(1)
    rows, cols = z_ref.shape
    chunks = g_even.shape[1] // cols

    def make_g(dst):
        begin = jnp.minimum(step, chunks - 1) * cols
        lane = lax.broadcasted_iota(jnp.int32, (1, LANES), 1) + begin
        for r in range(0, rows, PART):
            here = slice(r, r + PART)
            top, inv, lab, found = top_ref[here, :], inv_ref[here, :], lab_ref[here, :], hits[here, :]
            for c in range(0, cols, LANES):
                z = z_ref[here, c : c + LANES]
                hit = lane + c == lab
                found = jnp.where(hit, z, found)
                g = (jnp.exp(z - top) * inv - jnp.where(hit, inv_tokens, 0.0)).astype(BF16)
                g_ref[here, c : c + LANES] = g
                if dst is not None:
                    dst[here, pl.ds(pl.multiple_of(begin + c, LANES), LANES)] = g
            hits[here, :] = found

    def product(src):
        for r in range(0, rows, X_SUB):
            dx_ref[r : r + X_SUB, :] = lax.dot_general(
                src[r : r + X_SUB, :], w_ref[...], (((1,), (1,)), ((), ())), preferred_element_type=F32
            )

    @pl.when(step == 0)
    def _():
        hits[...] = jnp.zeros_like(hits)

    if resume:
        @pl.when((block == 0) & (step == 0))
        def _():
            fetch = pltpu.make_async_copy(g_in.at[pl.ds(first * rows, rows)], g_even, sem)
            fetch.start()
            fetch.wait()

        @pl.when(block == 0)
        def _():
            product(g_even)
            make_g(g_odd)

        @pl.when(block == 1)
        def _():
            product(g_odd)
    else:
        @pl.when((block == 0) & (step < chunks))
        def _():
            make_g(g_even)

        @pl.when(block == 1)
        def _():
            product(g_even)
            make_g(g_odd)

        @pl.when(block == 2)
        def _():
            product(g_odd)
            make_g(None)

    @pl.when(step == steps - 1)
    def _():
        hit_ref[...] = jnp.sum(hits[...].reshape(-1, 8, LANES), axis=0)


def grad_x_call(z, w, top, inv, lab, inv_tokens, g=None):
    total, vocab = z.shape
    hidden = w.shape[0]
    blocks = total // G_ROWS // 2
    assert blocks == 2
    resume = g is not None
    steps, chunks = hidden // X_TILE, vocab // G_COLS
    bound = lambda h: jnp.minimum(h, chunks - 1)
    if resume:
        grid = (blocks, steps)
        row = lambda i: 2 * blocks - 1
        chunk = lambda i, h: (row(i), jnp.where(i == 0, bound(h), chunks - 1))
        w_block = lambda i, h: (h, 0)
        dx_block = lambda i, h: (i, h)
    else:
        grid = (blocks + 1, steps)
        row = lambda i: i
        chunk = lambda i, h: (i, bound(h))
        w_block = lambda i, h: (jnp.where(i == 0, 0, h), 0)
        dx_block = lambda i, h: (jnp.maximum(i - 1, 0), jnp.where(i == 0, 0, h))
    stat = pl.BlockSpec((G_ROWS, LANES), lambda i, h: (row(i), 0))
    scratch = [pltpu.VMEM((G_ROWS, vocab), BF16)] * 2 + [pltpu.VMEM((G_ROWS, LANES), F32)]
    return pl.pallas_call(
        functools.partial(grad_x_kernel, first=blocks, blocks=blocks, inv_tokens=inv_tokens, resume=resume),
        grid=grid,
        in_specs=[pl.BlockSpec((G_ROWS, G_COLS), chunk), pl.BlockSpec((X_TILE, vocab), w_block), stat, stat, stat]
        + ([pl.BlockSpec(memory_space=pl.ANY)] if resume else []),
        out_specs=[
            pl.BlockSpec((G_ROWS, G_COLS), chunk),
            pl.BlockSpec((G_ROWS, X_TILE), dx_block),
            pl.BlockSpec((8, LANES), lambda i, h: (i, 0)),
        ],
        out_shape=[
            jax.ShapeDtypeStruct((total, vocab), BF16),
            jax.ShapeDtypeStruct((total // 2, hidden), F32),
            jax.ShapeDtypeStruct((8 * grid[0], LANES), F32),
        ],
        scratch_shapes=scratch + ([pltpu.SemaphoreType.DMA] if resume else []),
        input_output_aliases={5: 0} if resume else {},
        compiler_params=pltpu.CompilerParams(vmem_limit_bytes=VMEM_BYTES),
        cost_estimate=pl.CostEstimate(flops=total * hidden * vocab, bytes_accessed=3 * total * vocab, transcendentals=0),
        name="grad_x_b" if resume else "grad_x_a",
    )(z, w, top, inv, lab, *([g] if resume else []))


def solution(mesh):
    group = mesh.shape["tp"]

    def local_step(x_a, x_b, labels_a, labels_b, w):
        vocab = w.shape[1]
        tokens = x_a.shape[0] * group
        z, x_full, labels, stats = gather_logits(x_a, x_b, jnp.stack([labels_a, labels_b]), w, group)
        row_max = jnp.max(stats[:, :, 0], axis=0)
        row_sum = jnp.sum(stats[:, :, 1] * jnp.exp(stats[:, :, 0] - row_max), axis=0)
        labels = jnp.transpose(labels, (1, 0, 2)).reshape(-1) - lax.axis_index("tp") * vocab
        spread = lambda a: jnp.broadcast_to(a.reshape(-1, 1), (2 * tokens, LANES))
        top, inv, lab = spread(row_max), spread(1.0 / (row_sum * tokens)), spread(labels)
        g, part_a, hit_a = grad_x_call(z, w, top, inv, lab, 1.0 / tokens)
        grad_x_a = lax.psum_scatter(part_a, "tp", scatter_dimension=0, tiled=True).astype(BF16)
        g, part_b, hit_b = grad_x_call(z, w, top, inv, lab, 1.0 / tokens, g)
        grad_x_b = lax.psum_scatter(part_b, "tp", scatter_dimension=0, tiled=True).astype(BF16)
        own = jnp.stack([jnp.sum(hit_a[:16]), jnp.sum(hit_a[16:]) + jnp.sum(hit_b[:8])])
        target = lax.psum(own, "tp")
        losses = jnp.mean(row_max + jnp.log(row_sum), axis=-1) - target / tokens
        pair = lambda a: a.reshape(2, tokens, -1)
        grad_w = jnp.einsum("mth,mtv->hv", pair(x_full), pair(g), preferred_element_type=F32).astype(BF16)
        return losses, grad_w, grad_x_a, grad_x_b

    rows, labs = P(("dp", "tp"), None), P(("dp", "tp"))
    return jax.shard_map(
        local_step,
        mesh=mesh,
        in_specs=(rows, rows, labs, labs, P(None, "tp")),
        out_specs=(P("dp"), P("dp", "tp"), rows, rows),
        check_vma=False,
    )
```

```python
import functools

import jax
import jax.numpy as jnp
from jax import lax
from jax.experimental import pallas as pl
from jax.experimental.pallas import tpu as pltpu
from jax.sharding import PartitionSpec as P


F32 = jnp.float32
BF16 = jnp.bfloat16
LOWEST = -3.4028235e38
VMEM_BYTES = 67043328
LANES = 128
CHIPS = 4
PHASES = 2 * CHIPS
LOGIT_COLS, LOGIT_SUB = 1024, 512
G_ROWS, G_COLS, X_TILE, X_SUB, PART, MIX = 1024, 768, 512, 256, 8, 256
PARTNER, RIGHT, LEFT, FORWARD_RIGHT, FORWARD_LEFT, PASS_RIGHT, PASS_LEFT, PASS_FIRST, PASS_SECOND = range(9)


def phase_block(phase, chip):
    turn = lax.rem(phase + 1, 3)
    away = lax.min(lax.div(phase, 2), 1) * (1 + 2 * turn - 3 * lax.div(turn, 2))
    batch = lax.div(phase, 5) + 1 - lax.min((phase - 1) * (phase - 1), 1)
    return batch, lax.rem(chip + away, CHIPS)


def logits_kernel(
    x_a, x_b, lab, w_ref, z_ref, x_full, lab_full, stat_full,
    x_buf, run_max, run_sum, stat,
    send_sem, recv_sem, lab_send, lab_recv, stat_send, stat_recv, own_sem, keep_sem, load_sem,
    *, group, sub,
):
    phase, step = pl.program_id(0), pl.program_id(1)
    steps = pl.num_programs(1)
    rows, cols = z_ref.shape
    unit = x_a.shape[0]
    half = unit // 2
    tokens = unit * group
    me = lax.axis_index("tp")
    chip, core = lax.div(me, 2), lax.rem(me, 2)
    partner = chip * 2 + 1 - core
    device = lambda hops: lax.rem(chip + hops, CHIPS) * 2 + core
    right, opposite, left = device(1), device(2), device(3)
    x_own = (x_a, x_b)

    def rows_of(batch, dev, first=0, size=unit):
        return x_full.at[pl.ds(pl.multiple_of(batch * tokens + dev * unit + first, half), size)]

    def copy(kind, batch):
        src = dst = None
        if kind == PARTNER:
            src, to = x_own[batch], partner
            dst = x_buf.at[batch, pl.ds(pl.multiple_of(core * unit, half), unit)]
        elif kind in (RIGHT, LEFT):
            src, to = x_own[batch], right if kind == RIGHT else left
            dst = rows_of(batch, me)
        elif kind == FORWARD_RIGHT:
            src, to = rows_of(batch, left, 0, half), right
        elif kind == FORWARD_LEFT:
            src, to = rows_of(batch, right, half, half), left
        elif kind == PASS_RIGHT:
            src, to = rows_of(batch, right), partner
        elif kind == PASS_LEFT:
            src, to = rows_of(batch, left), partner
        elif kind == PASS_FIRST:
            src, to = rows_of(batch, opposite, 0, half), partner
        else:
            src, to = rows_of(batch, opposite, half, half), partner
        return pltpu.make_async_remote_copy(
            src_ref=src, dst_ref=src if dst is None else dst,
            send_sem=send_sem.at[kind, batch], recv_sem=recv_sem.at[kind, batch],
            device_id={"tp": to}, device_id_type=pl.DeviceIdType.MESH,
        )

    def label_copy(k):
        return pltpu.make_async_remote_copy(
            src_ref=lab, dst_ref=lab_full.at[me], send_sem=lab_send.at[k], recv_sem=lab_recv.at[k],
            device_id={"tp": lax.rem(me + k, group)}, device_id_type=pl.DeviceIdType.MESH,
        )

    def stat_copy(batch, k):
        return pltpu.make_async_remote_copy(
            src_ref=stat.at[batch], dst_ref=stat_full.at[me, batch],
            send_sem=stat_send.at[batch, k], recv_sem=stat_recv.at[batch, k],
            device_id={"tp": lax.rem(me + k, group)}, device_id_type=pl.DeviceIdType.MESH,
        )

    def own_load(batch):
        return pltpu.make_async_copy(
            x_own[batch], x_buf.at[batch, pl.ds(pl.multiple_of(core * unit, half), unit)], own_sem.at[batch]
        )

    def own_keep(batch):
        return pltpu.make_async_copy(x_buf.at[batch], rows_of(batch, chip * 2, 0, 2 * unit), keep_sem.at[batch])

    def load(to_phase):
        batch, away = phase_block(jnp.int32(to_phase), chip)
        return pltpu.make_async_copy(rows_of(batch, away * 2, 0, 2 * unit), x_buf.at[to_phase % 2], load_sem)

    label_own = pltpu.make_async_copy(lab, lab_full.at[me], own_sem.at[2])
    stat_own = lambda batch: pltpu.make_async_copy(stat.at[batch], stat_full.at[me, batch], own_sem.at[3 + batch])
    at = lambda p, s: pl.when((phase == p) & (step == s))
    last = steps - 1
    others = range(1, group)

    @at(0, 0)
    def _():
        barrier = pltpu.get_barrier_semaphore()
        for k in others:
            pl.semaphore_signal(
                barrier, inc=1, device_id={"tp": lax.rem(me + k, group)}, device_id_type=pl.DeviceIdType.MESH
            )
        own_load(0).start()
        own_load(1).start()
        pl.semaphore_wait(barrier, group - 1)
        copy(PARTNER, 0).start()
        copy(RIGHT, 0).start()
        copy(LEFT, 0).start()
        copy(PARTNER, 1).start()
        for k in others:
            label_copy(k).start()
        label_own.start()
        own_load(0).wait()
        copy(PARTNER, 0).wait_recv()
        own_keep(0).start()

    @at(0, last)
    def _():
        own_load(1).wait()
        copy(PARTNER, 1).wait_recv()
        own_keep(1).start()

    def arrived(batch):
        copy(RIGHT, batch).wait_recv()
        copy(LEFT, batch).wait_recv()
        copy(FORWARD_RIGHT, batch).start()
        copy(FORWARD_LEFT, batch).start()
        copy(PASS_RIGHT, batch).start()
        copy(PASS_LEFT, batch).start()

    def arrived_far(batch):
        copy(FORWARD_RIGHT, batch).wait_recv()
        copy(FORWARD_LEFT, batch).wait_recv()
        copy(PASS_FIRST, batch).start()
        copy(PASS_SECOND, batch).start()

    @at(1, (7 * steps) // 12)
    def _():
        arrived(0)
        copy(RIGHT, 1).start()
        copy(LEFT, 1).start()

    @at(1, last)
    def _():
        own_keep(0).wait()
        copy(PASS_RIGHT, 0).wait_recv()
        load(2).start()

    @at(2, (8 * steps) // 12)
    def _():
        arrived_far(0)

    @at(2, last)
    def _():
        own_keep(1).wait()
        copy(PASS_LEFT, 0).wait_recv()
        load(3).start()

    @at(3, last)
    def _():
        copy(PASS_FIRST, 0).wait_recv()
        copy(PASS_SECOND, 0).wait_recv()
        load(4).start()

    @at(4, (4 * steps) // 12)
    def _():
        arrived(1)

    @at(4, last)
    def _():
        copy(PASS_RIGHT, 1).wait_recv()
        load(5).start()

    @at(5, 1)
    def _():
        for k in others:
            stat_copy(0, k).start()
        stat_own(0).start()

    @at(5, (6 * steps) // 12)
    def _():
        arrived_far(1)

    @at(5, last)
    def _():
        copy(PASS_LEFT, 1).wait_recv()
        load(6).start()

    @at(6, last)
    def _():
        copy(PASS_FIRST, 1).wait_recv()
        copy(PASS_SECOND, 1).wait_recv()
        load(7).start()

    @pl.when((step == 0) & (phase >= 2))
    def _():
        load(2).wait()

    @pl.when(step == 0)
    def _():
        run_max[...] = jnp.full_like(run_max, LOWEST)
        run_sum[...] = jnp.zeros_like(run_sum)

    x = x_buf.at[lax.rem(phase, 2)]
    for r in range(0, rows, sub):
        tile = jnp.dot(x[r : r + sub, :], w_ref[...], preferred_element_type=F32)
        z_ref[r : r + sub, :] = tile
        old = run_max[r : r + sub, :]
        new = old
        for c in range(0, cols, LANES):
            new = jnp.maximum(new, tile[:, c : c + LANES])
        total = run_sum[r : r + sub, :] * jnp.exp(old - new)
        for c in range(0, cols, LANES):
            total = total + jnp.exp(tile[:, c : c + LANES] - new)
        run_max[r : r + sub, :] = new
        run_sum[r : r + sub, :] = total

    @pl.when(step == last)
    def _():
        batch, away = phase_block(phase, chip)
        spot = pl.ds(pl.multiple_of(away * rows, rows), rows)
        lane_max = run_max[...].T
        top = jnp.max(lane_max, axis=0, keepdims=True)
        stat[batch, 0:1, spot] = top
        stat[batch, 1:2, spot] = jnp.sum(run_sum[...].T * jnp.exp(lane_max - top), axis=0, keepdims=True)

    @at(PHASES - 1, last)
    def _():
        for kind in range(9):
            for batch in range(2):
                copy(kind, batch).wait_send()
        for k in others:
            label_copy(k).wait()
        label_own.wait()
        for k in others:
            stat_copy(1, k).start()
        stat_own(1).start()
        for batch in range(2):
            for k in others:
                stat_copy(batch, k).wait()
            stat_own(batch).wait()


def gather_logits(x_a, x_b, lab, w, group):
    unit, hidden = x_a.shape
    vocab = w.shape[1]
    tokens = unit * group
    rows, cols, sub = 2 * unit, LOGIT_COLS, LOGIT_SUB

    def z_block(phase, step):
        batch, away = phase_block(phase, lax.div(lax.axis_index("tp"), 2))
        return batch * CHIPS + away, step

    hbm = pl.BlockSpec(memory_space=pl.ANY)
    dma = pltpu.SemaphoreType.DMA
    return pl.pallas_call(
        functools.partial(logits_kernel, group=group, sub=sub),
        grid=(PHASES, vocab // cols),
        in_specs=[hbm, hbm, hbm, pl.BlockSpec((hidden, cols), lambda p, n: (0, n))],
        out_specs=[pl.BlockSpec((rows, cols), z_block), hbm, hbm, hbm],
        out_shape=[
            jax.ShapeDtypeStruct((2 * tokens, vocab), F32),
            jax.ShapeDtypeStruct((2 * tokens, hidden), BF16),
            jax.ShapeDtypeStruct((group, 2, unit), jnp.int32),
            jax.ShapeDtypeStruct((group, 2, 2, tokens), F32),
        ],
        scratch_shapes=[
            pltpu.VMEM((2, rows, hidden), BF16),
            pltpu.VMEM((rows, LANES), F32),
            pltpu.VMEM((rows, LANES), F32),
            pltpu.VMEM((2, 2, tokens), F32),
            dma((9, 2)), dma((9, 2)), dma((group,)), dma((group,)), dma((2, group)), dma((2, group)),
            dma((5,)), dma((2,)), dma,
        ],
        compiler_params=pltpu.CompilerParams(
            vmem_limit_bytes=VMEM_BYTES, collective_id=0, has_side_effects=True,
            dimension_semantics=("arbitrary", "arbitrary"),
        ),
        cost_estimate=pl.CostEstimate(
            flops=4 * tokens * hidden * vocab, bytes_accessed=8 * tokens * vocab, transcendentals=0
        ),
        name="gather_logits",
    )(x_a, x_b, lab, w)


def share_kernel(own, all_ref, send_sem, recv_sem, keep_sem, *, group):
    me = lax.axis_index("tp")
    others = range(1, group)

    def copy(k):
        return pltpu.make_async_remote_copy(
            src_ref=own, dst_ref=all_ref.at[me], send_sem=send_sem.at[k], recv_sem=recv_sem.at[k],
            device_id={"tp": lax.rem(me + k, group)}, device_id_type=pl.DeviceIdType.MESH,
        )

    barrier = pltpu.get_barrier_semaphore()
    for k in others:
        pl.semaphore_signal(
            barrier, inc=1, device_id={"tp": lax.rem(me + k, group)}, device_id_type=pl.DeviceIdType.MESH
        )
    pl.semaphore_wait(barrier, group - 1)
    for k in others:
        copy(k).start()
    keep = pltpu.make_async_copy(own, all_ref.at[me], keep_sem)
    keep.start()
    keep.wait()
    for k in others:
        copy(k).wait()


def share(own, group):
    hbm = pl.BlockSpec(memory_space=pl.ANY)
    dma = pltpu.SemaphoreType.DMA
    return pl.pallas_call(
        functools.partial(share_kernel, group=group),
        in_specs=[hbm],
        out_specs=hbm,
        out_shape=jax.ShapeDtypeStruct((group, *own.shape), own.dtype),
        scratch_shapes=[dma((group,)), dma((group,)), dma],
        compiler_params=pltpu.CompilerParams(collective_id=1, has_side_effects=True),
        name="share",
    )(own)


def grad_x_kernel(*refs, first, inv_tokens, resume):
    if resume:
        z_ref, w_ref, top_ref, inv_ref, lab_ref, g_in, g_ref, dx_ref, hit_ref, g_even, g_odd, hits, sem = refs
    else:
        z_ref, w_ref, top_ref, inv_ref, lab_ref, g_ref, dx_ref, hit_ref, g_even, g_odd, hits = refs
    block, step = pl.program_id(0), pl.program_id(1)
    steps = pl.num_programs(1)
    rows, cols = z_ref.shape
    chunks = g_even.shape[1] // cols

    def make_g(dst, low=0, high=None):
        begin = jnp.minimum(step, chunks - 1) * cols
        lane = lax.broadcasted_iota(jnp.int32, (1, LANES), 1) + begin
        for r in range(low, rows if high is None else high, PART):
            here = slice(r, r + PART)
            top, inv, lab, found = top_ref[here, :], inv_ref[here, :], lab_ref[here, :], hits[here, :]
            for c in range(0, cols, LANES):
                z = z_ref[here, c : c + LANES]
                hit = lane + c == lab
                found = jnp.where(hit, z, found)
                g = (jnp.exp(z - top) * inv - jnp.where(hit, inv_tokens, 0.0)).astype(BF16)
                g_ref[here, c : c + LANES] = g
                if dst is not None:
                    dst[here, pl.ds(pl.multiple_of(begin + c, LANES), LANES)] = g
            hits[here, :] = found

    def product(src, low=0, high=None):
        for r in range(low, rows if high is None else high, X_SUB):
            dx_ref[r : r + X_SUB, :] = lax.dot_general(
                src[r : r + X_SUB, :], w_ref[...], (((1,), (1,)), ((), ())), preferred_element_type=F32
            )

    def both(src, dst):
        for r in range(0, rows, MIX):
            product(src, r, r + MIX)
            make_g(dst, r, r + MIX)

    @pl.when(step == 0)
    def _():
        hits[...] = jnp.zeros_like(hits)

    if resume:
        @pl.when((block == 0) & (step == 0))
        def _():
            fetch = pltpu.make_async_copy(g_in.at[pl.ds(first * rows, rows)], g_even, sem)
            fetch.start()
            fetch.wait()

        @pl.when(block == 0)
        def _():
            both(g_even, g_odd)

        @pl.when(block == 1)
        def _():
            product(g_odd)
    else:
        @pl.when((block == 0) & (step < chunks))
        def _():
            make_g(g_even)

        @pl.when(block == 1)
        def _():
            both(g_even, g_odd)

        @pl.when(block == 2)
        def _():
            both(g_odd, None)

    @pl.when(step == steps - 1)
    def _():
        hit_ref[...] = jnp.sum(hits[...].reshape(-1, 8, LANES), axis=0)


def grad_x_call(z, w, top, inv, lab, inv_tokens, g=None):
    total, vocab = z.shape
    hidden = w.shape[0]
    blocks = total // G_ROWS // 2
    assert blocks == 2
    resume = g is not None
    steps, chunks = hidden // X_TILE, vocab // G_COLS
    bound = lambda h: jnp.minimum(h, chunks - 1)
    if resume:
        grid = (blocks, steps)
        row = lambda i: 2 * blocks - 1
        chunk = lambda i, h: (row(i), jnp.where(i == 0, bound(h), chunks - 1))
        w_block = lambda i, h: (h, 0)
        dx_block = lambda i, h: (i, h)
    else:
        grid = (blocks + 1, steps)
        row = lambda i: i
        chunk = lambda i, h: (i, bound(h))
        w_block = lambda i, h: (jnp.where(i == 0, 0, h), 0)
        dx_block = lambda i, h: (jnp.maximum(i - 1, 0), jnp.where(i == 0, 0, h))
    stat = pl.BlockSpec((G_ROWS, LANES), lambda i, h: (row(i), 0))
    scratch = [pltpu.VMEM((G_ROWS, vocab), BF16)] * 2 + [pltpu.VMEM((G_ROWS, LANES), F32)]
    return pl.pallas_call(
        functools.partial(grad_x_kernel, first=blocks, inv_tokens=inv_tokens, resume=resume),
        grid=grid,
        in_specs=[pl.BlockSpec((G_ROWS, G_COLS), chunk), pl.BlockSpec((X_TILE, vocab), w_block), stat, stat, stat]
        + ([pl.BlockSpec(memory_space=pl.ANY)] if resume else []),
        out_specs=[
            pl.BlockSpec((G_ROWS, G_COLS), chunk),
            pl.BlockSpec((G_ROWS, X_TILE), dx_block),
            pl.BlockSpec((8, LANES), lambda i, h: (i, 0)),
        ],
        out_shape=[
            jax.ShapeDtypeStruct((total, vocab), BF16),
            jax.ShapeDtypeStruct((total // 2, hidden), F32),
            jax.ShapeDtypeStruct((8 * grid[0], LANES), F32),
        ],
        scratch_shapes=scratch + ([pltpu.SemaphoreType.DMA] if resume else []),
        input_output_aliases={5: 0} if resume else {},
        compiler_params=pltpu.CompilerParams(vmem_limit_bytes=VMEM_BYTES),
        cost_estimate=pl.CostEstimate(flops=total * hidden * vocab, bytes_accessed=3 * total * vocab, transcendentals=0),
        name="grad_x_b" if resume else "grad_x_a",
    )(z, w, top, inv, lab, *([g] if resume else []))


def solution(mesh):
    group = mesh.shape["tp"]

    def local_step(x_a, x_b, labels_a, labels_b, w):
        vocab = w.shape[1]
        tokens = x_a.shape[0] * group
        z, x_full, labels, stats = gather_logits(x_a, x_b, jnp.stack([labels_a, labels_b]), w, group)
        row_max = jnp.max(stats[:, :, 0], axis=0)
        row_sum = jnp.sum(stats[:, :, 1] * jnp.exp(stats[:, :, 0] - row_max), axis=0)
        labels = jnp.transpose(labels, (1, 0, 2)).reshape(-1) - lax.axis_index("tp") * vocab
        spread = lambda a: jnp.broadcast_to(a.reshape(-1, 1), (2 * tokens, LANES))
        top, inv, lab = spread(row_max), spread(1.0 / (row_sum * tokens)), spread(labels)
        g, part_a, hit_a = grad_x_call(z, w, top, inv, lab, 1.0 / tokens)
        sum_a = lax.psum_scatter(part_a, "tp", scatter_dimension=0, tiled=True)
        g, part_b, hit_b = grad_x_call(z, w, top, inv, lab, 1.0 / tokens, g)
        sum_b = lax.psum_scatter(part_b, "tp", scatter_dimension=0, tiled=True)
        grad_x_a, grad_x_b = sum_a.astype(BF16), sum_b.astype(BF16)
        own = jnp.stack([jnp.sum(hit_a[:16]), jnp.sum(hit_a[16:]) + jnp.sum(hit_b[:8])])
        shared = share(jnp.broadcast_to(own[:, None, None], (2, 8, LANES)), group)
        target = jnp.sum(shared[:, :, 0, 0], axis=0)
        losses = jnp.mean(row_max + jnp.log(row_sum), axis=-1) - target / tokens
        pair = lambda a: a.reshape(2, tokens, -1)
        grad_w = jnp.einsum("mth,mtv->hv", pair(x_full), pair(g), preferred_element_type=F32).astype(BF16)
        return losses, grad_w, grad_x_a, grad_x_b

    rows, labs = P(("dp", "tp"), None), P(("dp", "tp"))
    return jax.shard_map(
        local_step,
        mesh=mesh,
        in_specs=(rows, rows, labs, labs, P(None, "tp")),
        out_specs=(P("dp"), P("dp", "tp"), rows, rows),
        check_vma=False,
    )
```
